32 devices in a mesh: row: 16 (over z, y, core), rows: 2 (over x).
Axes of the slice: x: 2, y: 2, z: 4, core: 2. Of those that a mesh axis runs over, the one named last changes fastest.
Arguments:
- hopping: float32 [2, 128, 512, 512], P(None, 'row', 'rows'), may hold values from -0.5 to 0.5
- lattice: int32 [3, 128], replicated, may hold values from -4 to 4
- kgrid: int32 [3, 32], replicated, may hold values from 0 to 7
- tangent: float32 [3, 32], replicated, may hold values from -4 to 4
- states: float32 [2, 32, 1024, 512], P(None, 'row'), may hold values from -6 to 6
Outputs:
- energies: float32 [32, 1024], P('row')
- velocities: float32 [32, 1024], P('row')
The draws below stay inside these ranges and needn't reach their ends.
All inputs are finite; a program needn't handle non-finite values.
Results may differ from the reference program's by a relative error of at most 0.000075.
Values sent between devices are 32-bit elements; how exact they have to be, the bound alone decides.
A program may use at most 256 MiB of HBM per device.

```python
import math
import jax
import jax.numpy as jnp
from jax import lax

NW = 512
NR = 128
NB = 1024
K = 32
KGRID = 8


def with_ends(result, rng, smallest, high):
    dims = result.shape
    place = [jax.random.randint(jax.random.fold_in(rng, axis), (), 0, dims[axis]) for axis in range(len(dims))]
    result = result.at[tuple(place)].set(smallest)
    longest = dims.index(max(dims))
    place[longest] = (place[longest] + 1) % dims[longest]
    return result.at[tuple(place)].set(high)


def level_of(key, dims, cuts, least, high):
    factor_of, own = 1.0, jax.random.fold_in(key, 6)
    for dim, parts in cuts:
        steps = jnp.exp(jax.random.uniform(jax.random.fold_in(own, dim), (parts,), jnp.float32, least / len(cuts), high / len(cuts)))
        factor_of = factor_of * jnp.repeat(steps, dims[dim] // parts).reshape([-1 if axis == dim else 1 for axis in range(len(dims))])
    return factor_of


def scatter_about(stream_key, shape, spread, bound, pieces=(), held_as=jnp.bfloat16):
    factor_of = level_of(stream_key, shape, pieces, -0.22, 0.18) if pieces else 1.0
    values = jax.random.normal(stream_key, shape, jnp.float32) * spread * factor_of
    return jnp.minimum(jnp.maximum(values, -bound), bound).astype(held_as)


def setup_inputs(seed: int = 0) -> dict:
    splits = jax.random.split(jax.random.key(seed), 6)
    hopping = scatter_about(splits[0], (2, NR, NW, NW), NR ** -0.5, 0.5, ((1, 16), (2, 2)), jnp.float32)
    lattice = with_ends(jax.random.randint(splits[1], (3, NR), -4, 5), jax.random.fold_in(splits[1], 1), -4, 4).astype(jnp.int32)
    kgrid = with_ends(jax.random.randint(splits[2], (3, K), 0, KGRID), jax.random.fold_in(splits[2], 1), 0, KGRID - 1).astype(jnp.int32)
    tangent = scatter_about(splits[3], (3, K), 0.3, 4.0, (), jnp.float32)
    states = scatter_about(splits[4], (2, K, NB, NW), 1.0, 6.0, ((1, 16),), jnp.float32)
    return {"hopping": hopping, "lattice": lattice, "kgrid": kgrid, "tangent": tangent, "states": states}


def phases(kgrid, lattice, tangent):
    turns = jnp.mod(jnp.sum(kgrid[:, :, None] * lattice[:, None, :], axis=0), KGRID)
    angle = turns.astype(jnp.float32) * (2.0 * math.pi / KGRID)
    weight = jnp.sum(tangent[:, :, None] * lattice[:, None, :].astype(jnp.float32), axis=0)
    return jnp.cos(angle), jnp.sin(angle), weight


def expand(first, second, hopping):
    real_sum = jnp.einsum("kr,rab->kab", first, hopping[0], precision=lax.Precision.HIGHEST)
    imag_sum = jnp.einsum("kr,rab->kab", second, hopping[1], precision=lax.Precision.HIGHEST)
    cross_one = jnp.einsum("kr,rab->kab", second, hopping[0], precision=lax.Precision.HIGHEST)
    cross_two = jnp.einsum("kr,rab->kab", first, hopping[1], precision=lax.Precision.HIGHEST)
    return real_sum - imag_sum, cross_one + cross_two


def project(m_re, m_im, rows, cols):
    high = lax.Precision.HIGHEST
    y_re = jnp.einsum("kac,kic->kai", m_re, cols[0], precision=high) - jnp.einsum("kac,kic->kai", m_im, cols[1], precision=high)
    y_im = jnp.einsum("kac,kic->kai", m_re, cols[1], precision=high) + jnp.einsum("kac,kic->kai", m_im, cols[0], precision=high)
    return jnp.einsum("kia,kai->ki", rows[0], y_re, precision=high) + jnp.einsum("kia,kai->ki", rows[1], y_im, precision=high)


def reference(hopping, lattice, kgrid, tangent, states):
    cosine, sine, weight = phases(kgrid, lattice, tangent)
    hk_re, hk_im = expand(cosine, sine, hopping)
    dk_re, dk_im = expand(-weight * sine, weight * cosine, hopping)
    p_h = project(hk_re, hk_im, states, states)
    p_d = project(dk_re, dk_im, states, states)
    norm = jnp.sum(states[0] * states[0] + states[1] * states[1], axis=-1)
    return p_h / norm, p_d / norm
```

```python
import math

import jax
import jax.numpy as jnp
from jax import lax
from jax.sharding import PartitionSpec as P

KGRID = 8


def phases(kgrid, lattice, tangent):
    turns = jnp.mod(jnp.sum(kgrid[:, :, None] * lattice[:, None, :], axis=0), KGRID)
    angle = turns.astype(jnp.float32) * (2.0 * math.pi / KGRID)
    weight = jnp.sum(tangent[:, :, None] * lattice[:, None, :].astype(jnp.float32), axis=0)
    return (jnp.cos(angle), jnp.sin(angle), weight)


def project(m_re, m_im, rows, cols):
    high = lax.Precision.HIGH
    y_re = jnp.einsum("kmac,kic->kmai", m_re, cols[0], precision=high) - jnp.einsum(
        "kmac,kic->kmai", m_im, cols[1], precision=high
    )
    y_im = jnp.einsum("kmac,kic->kmai", m_re, cols[1], precision=high) + jnp.einsum(
        "kmac,kic->kmai", m_im, cols[0], precision=high
    )
    a = jnp.swapaxes(rows[0], 1, 2)[:, None]
    b = jnp.swapaxes(rows[1], 1, 2)[:, None]
    return jnp.sum(a * y_re + b * y_im, axis=2)


def per_device(hopping, lattice, kgrid, tangent, states):
    row_count = hopping.shape[2]
    row_start = lax.axis_index("rows") * row_count
    state_rows = lax.dynamic_slice_in_dim(states, row_start, row_count, 3)
    cosine, sine, weight = phases(kgrid, lattice, tangent)
    slab = lax.all_to_all(hopping, "row", 2, 1, tiled=True)
    first_d, second_d = -weight * sine, weight * cosine
    coef = jnp.stack(
        [
            jnp.stack([cosine, -sine], axis=1),
            jnp.stack([sine, cosine], axis=1),
            jnp.stack([first_d, -second_d], axis=1),
            jnp.stack([second_d, first_d], axis=1),
        ],
        axis=1,
    )
    blocks = jnp.einsum("kmpr,prac->kmac", coef, slab, precision=lax.Precision.HIGHEST)
    tiles = lax.all_to_all(blocks, "row", 0, 2, tiled=True)
    m_re = tiles[:, 0::2]
    m_im = tiles[:, 1::2]
    pieces = project(m_re, m_im, state_rows, states)
    totals = lax.psum(pieces, "rows")
    norm = jnp.sum(states[0] * states[0] + states[1] * states[1], axis=-1)
    return (totals[:, 0] / norm, totals[:, 1] / norm)


def solution(mesh):
    placed = (P(None, "row", "rows", None), P(), P(), P(), P(None, "row", None, None))
    return jax.shard_map(
        per_device,
        mesh=mesh,
        in_specs=placed,
        out_specs=(P("row", None), P("row", None)),
        check_vma=False,
    )
```

```python
import math

import jax
import jax.numpy as jnp
from jax import lax
from jax.sharding import PartitionSpec as P

KGRID = 8


def phases(kgrid, lattice, tangent):
    turns = jnp.mod(jnp.sum(kgrid[:, :, None] * lattice[:, None, :], axis=0), KGRID)
    angle = turns.astype(jnp.float32) * (2.0 * math.pi / KGRID)
    weight = jnp.sum(tangent[:, :, None] * lattice[:, None, :].astype(jnp.float32), axis=0)
    return (jnp.cos(angle), jnp.sin(angle), weight)


def project(m_re, m_im, rows, cols):
    high = lax.Precision.HIGH
    y_re = jnp.einsum("kmac,kic->kmai", m_re, cols[0], precision=high) - jnp.einsum(
        "kmac,kic->kmai", m_im, cols[1], precision=high
    )
    y_im = jnp.einsum("kmac,kic->kmai", m_re, cols[1], precision=high) + jnp.einsum(
        "kmac,kic->kmai", m_im, cols[0], precision=high
    )
    a = jnp.swapaxes(rows[0], 1, 2)[:, None]
    b = jnp.swapaxes(rows[1], 1, 2)[:, None]
    return jnp.sum(a * y_re + b * y_im, axis=2)


def per_device(hopping, lattice, kgrid, tangent, states):
    row_count = hopping.shape[2]
    row_start = lax.axis_index("rows") * row_count
    state_rows = lax.dynamic_slice_in_dim(states, row_start, row_count, 3)
    cosine, sine, weight = phases(kgrid, lattice, tangent)
    first_d, second_d = -weight * sine, weight * cosine
    coef = jnp.stack(
        [
            jnp.stack([cosine, -sine], axis=1),
            jnp.stack([sine, cosine], axis=1),
            jnp.stack([first_d, -second_d], axis=1),
            jnp.stack([second_d, first_d], axis=1),
        ],
        axis=1,
    )
    halves = 2 if row_count % (2 * lax.axis_size("row")) == 0 else 1
    part = row_count // halves
    slabs = [
        lax.all_to_all(hopping[:, :, h * part : (h + 1) * part], "row", 2, 1, tiled=True)
        for h in range(halves)
    ]
    tiles = []
    for slab in slabs:
        blocks = jnp.einsum("kmpr,prac->kmac", coef, slab, precision=lax.Precision.HIGHEST)
        tiles.append(lax.all_to_all(blocks, "row", 0, 2, tiled=True))
    pieces = 0.0
    for h, tile in enumerate(tiles):
        rows = state_rows[..., h * part : (h + 1) * part]
        pieces = pieces + project(tile[:, 0::2], tile[:, 1::2], rows, states)
    totals = lax.psum(pieces, "rows")
    norm = jnp.sum(states[0] * states[0] + states[1] * states[1], axis=-1)
    return (totals[:, 0] / norm, totals[:, 1] / norm)


def solution(mesh):
    placed = (P(None, "row", "rows", None), P(), P(), P(), P(None, "row", None, None))
    return jax.shard_map(
        per_device,
        mesh=mesh,
        in_specs=placed,
        out_specs=(P("row", None), P("row", None)),
        check_vma=False,
    )
```
